8 devices in a mesh: cp: 8 (over z, y, x, core).
Axes of the slice: x: 2, y: 2, z: 1, core: 2. Of those that a mesh axis runs over, the one named last changes fastest.
Arguments:
- x_in: bfloat16 [3, 4096, 2048], P(None, 'cp')
- grad_y: bfloat16 [3, 4096, 2048], P(None, 'cp')
- positions: int32 [3, 4096], P(None, 'cp')
- norm_gain: bfloat16 [2048], replicated
- w_query: bfloat16 [2048, 2048], replicated
- w_key: bfloat16 [2048, 1024], replicated
- w_value: bfloat16 [2048, 1024], replicated
- w_out: bfloat16 [2048, 2048], replicated
- q_gain: bfloat16 [128], replicated
- k_gain: bfloat16 [128], replicated
Outputs:
- output 1: bfloat16 [3, 4096, 2048], P(None, 'cp')
- output 2: bfloat16 [3, 4096, 2048], P(None, 'cp')
- output 3: float32 [2048], replicated
- output 4: float32 [2048, 2048], replicated
- output 5: float32 [2048, 1024], replicated
- output 6: float32 [2048, 1024], replicated
- output 7: float32 [2048, 2048], replicated
- output 8: float32 [128], replicated
- output 9: float32 [128], replicated
All inputs are finite; a program needn't handle non-finite values.
Results may differ from the reference program's by a relative error of at most 0.0178088.
Values are sent between devices in bfloat16 or wider.
A program may use at most 1 GiB of HBM per device.

```python
import jax
import jax.numpy as jnp
from jax import lax

N_BATCH = 3
SEQ_LEN = 4096
MODEL_DIM = 2048
N_HEADS = 16
KV_HEADS = 8
HEAD_DIM = 128
Q_ROWS = 32
ROPE_THETA = 1000000.0
EPSILON = 1e-6
MASK_VALUE = -1e30


def setup_inputs(seed: int = 0) -> dict:
    rng_keys = jax.random.split(jax.random.key(seed), 11)
    q_width = N_HEADS * HEAD_DIM
    kv_width = KV_HEADS * HEAD_DIM
    tok_shape = (N_BATCH, SEQ_LEN, MODEL_DIM)
    x_in = jax.random.normal(rng_keys[0], tok_shape, jnp.float32)
    grad_y = jax.random.normal(rng_keys[1], tok_shape, jnp.float32)
    pos_gaps = jax.random.randint(rng_keys[2], (N_BATCH, SEQ_LEN), 1, 3)
    start_offsets = jax.random.randint(rng_keys[3], (N_BATCH, 1), 0, 1024)
    positions = start_offsets + jnp.cumsum(pos_gaps, axis=1) - 1
    norm_gain = 1.0 + 0.3 * jax.random.normal(rng_keys[4], (MODEL_DIM,), jnp.float32)
    w_query = jax.random.normal(rng_keys[5], (MODEL_DIM, q_width), jnp.float32) * MODEL_DIM ** -0.5
    w_key = jax.random.normal(rng_keys[6], (MODEL_DIM, kv_width), jnp.float32) * MODEL_DIM ** -0.5
    w_value = jax.random.normal(rng_keys[7], (MODEL_DIM, kv_width), jnp.float32) * MODEL_DIM ** -0.5
    w_out = jax.random.normal(rng_keys[8], (q_width, MODEL_DIM), jnp.float32) * q_width ** -0.5
    q_gain = 1.4 + 0.4 * jax.random.normal(rng_keys[9], (HEAD_DIM,), jnp.float32)
    k_gain = 1.4 + 0.4 * jax.random.normal(rng_keys[10], (HEAD_DIM,), jnp.float32)
    return {
        'x_in': x_in.astype(jnp.bfloat16),
        'grad_y': grad_y.astype(jnp.bfloat16),
        'positions': positions.astype(jnp.int32),
        'norm_gain': norm_gain.astype(jnp.bfloat16),
        'w_query': w_query.astype(jnp.bfloat16),
        'w_key': w_key.astype(jnp.bfloat16),
        'w_value': w_value.astype(jnp.bfloat16),
        'w_out': w_out.astype(jnp.bfloat16),
        'q_gain': q_gain.astype(jnp.bfloat16),
        'k_gain': k_gain.astype(jnp.bfloat16),
    }


def cast_down(t_val):
    return t_val.astype(jnp.bfloat16).astype(jnp.float32)


def rope_tables(positions):
    half_dim = HEAD_DIM // 2
    inv_freq = ROPE_THETA ** (-jnp.arange(half_dim, dtype=jnp.float32) / half_dim)
    angles = positions.astype(jnp.float32)[:, :, None] * inv_freq
    return jnp.cos(angles)[:, :, None, :], jnp.sin(angles)[:, :, None, :]


def head_prep(t_lin, gain, cos_t, sin_t):
    half_dim = HEAD_DIM // 2
    normed = t_lin * lax.rsqrt(jnp.mean(t_lin * t_lin, axis=-1, keepdims=True) + EPSILON) * gain
    lower_half = normed[..., :half_dim]
    upper_half = normed[..., half_dim:]
    return jnp.concatenate([lower_half * cos_t - upper_half * sin_t, upper_half * cos_t + lower_half * sin_t], axis=-1)


def causal_attention(q_rot, k_rot, v_lin):
    group_size = N_HEADS // KV_HEADS
    n_blocks = SEQ_LEN // Q_ROWS
    score_scale = HEAD_DIM ** -0.5
    q_blocks = jnp.moveaxis(q_rot.reshape(N_BATCH, n_blocks, Q_ROWS, KV_HEADS, group_size, HEAD_DIM), 1, 0)
    key_ids = jnp.arange(SEQ_LEN)

    def one_block(operands):
        q_blk, blk_index = operands
        scores = jnp.einsum('bqkgd,bskd->bqkgs', q_blk, k_rot) * score_scale
        query_ids = blk_index * Q_ROWS + jnp.arange(Q_ROWS)
        allowed = (key_ids[None, :] <= query_ids[:, None])[None, :, None, None, :]
        scores = jnp.where(allowed, scores, MASK_VALUE)
        probs = cast_down(jax.nn.softmax(scores, axis=-1))
        return jnp.einsum('bqkgs,bskd->bqkgd', probs, v_lin)

    block_outs = lax.map(jax.checkpoint(one_block), (q_blocks, jnp.arange(n_blocks)))
    return jnp.moveaxis(block_outs, 0, 1).reshape(N_BATCH, SEQ_LEN, N_HEADS * HEAD_DIM)


def block_forward(x32, positions, norm_gain, w_query, w_key, w_value, w_out, q_gain, k_gain):
    cos_t, sin_t = rope_tables(positions)
    inv_rms = lax.rsqrt(jnp.mean(x32 * x32, axis=-1, keepdims=True) + EPSILON)
    normed = cast_down(x32 * inv_rms * norm_gain)
    q_lin = jnp.einsum('bsd,de->bse', normed, w_query).reshape(N_BATCH, SEQ_LEN, N_HEADS, HEAD_DIM)
    k_lin = jnp.einsum('bsd,de->bse', normed, w_key).reshape(N_BATCH, SEQ_LEN, KV_HEADS, HEAD_DIM)
    v_lin = cast_down(jnp.einsum('bsd,de->bse', normed, w_value)).reshape(N_BATCH, SEQ_LEN, KV_HEADS, HEAD_DIM)
    q_rot = cast_down(head_prep(q_lin, q_gain, cos_t, sin_t))
    k_rot = cast_down(head_prep(k_lin, k_gain, cos_t, sin_t))
    attn = cast_down(causal_attention(q_rot, k_rot, v_lin))
    return x32 + jnp.einsum('bse,ed->bsd', attn, w_out)


def reference(x_in, grad_y, positions, norm_gain, w_query, w_key, w_value, w_out, q_gain, k_gain):
    x32 = x_in.astype(jnp.float32)
    gain32 = norm_gain.astype(jnp.float32)
    w_query32 = w_query.astype(jnp.float32)
    w_key32 = w_key.astype(jnp.float32)
    w_value32 = w_value.astype(jnp.float32)
    w_out32 = w_out.astype(jnp.float32)
    q_gain32 = q_gain.astype(jnp.float32)
    k_gain32 = k_gain.astype(jnp.float32)

    def block_fn(x_val, gain_val, wq_val, wk_val, wv_val, wo_val, qg_val, kg_val):
        return block_forward(x_val, positions, gain_val, wq_val, wk_val, wv_val, wo_val, qg_val, kg_val)

    y_out, pullback = jax.vjp(block_fn, x32, gain32, w_query32, w_key32, w_value32, w_out32, q_gain32, k_gain32)
    grads = pullback(grad_y.astype(jnp.float32))
    return (y_out.astype(jnp.bfloat16), grads[0].astype(jnp.bfloat16), grads[1], grads[2], grads[3], grads[4], grads[5], grads[6], grads[7])
```

```python
import functools

import jax
import jax.numpy as jnp
from jax import lax
from jax.experimental import pallas as pl
from jax.experimental.pallas import tpu as pltpu
from jax.sharding import PartitionSpec as P

SEQ_AXIS = 'cp'
ROPE_THETA = 1000000.0
EPSILON = 1e-6
MASK_VALUE = -1e30
LOG2E = 1.4426950408889634
HD = 128
BLK = 512
F32 = jnp.float32
BF16 = jnp.bfloat16
VMEM_LIMIT = 60 * 1024 * 1024


def dot_nn(a, b):
    return lax.dot_general(a, b, (((1,), (0,)), ((), ())), preferred_element_type=F32)


def dot_nt(a, b):
    return lax.dot_general(a, b, (((1,), (1,)), ((), ())), preferred_element_type=F32)


def prep(t, gain, cos, sin):
    r = lax.rsqrt(jnp.mean(t * t, axis=-1, keepdims=True) + EPSILON)
    normed = t * r * gain
    return normed * cos + pltpu.roll(normed, HD // 2, 1) * sin


def prep_back(d_rot, t, gain, cos, sin):
    d_norm = d_rot * cos - pltpu.roll(d_rot, HD // 2, 1) * sin
    r = lax.rsqrt(jnp.mean(t * t, axis=-1, keepdims=True) + EPSILON)
    d_gain = jnp.sum(d_norm * (t * r), axis=0, keepdims=True)
    scaled = d_norm * gain
    dot_mean = jnp.mean(scaled * t, axis=-1, keepdims=True)
    return r * scaled - t * (r * r * r * dot_mean), d_gain


def proj_kernel(n_ref, w_ref, cos_ref, sin_ref, qg_ref, kg_ref, q_ref, qt_ref, k_ref, kt_ref, v_ref, vt_ref, lin_ref):
    lin = dot_nn(n_ref[...], w_ref[...])
    lin_ref[...] = lin[:, :3 * HD]
    cos, sin = cos_ref[...], sin_ref[...]
    for h in range(2):
        q = prep(lin[:, h * HD:(h + 1) * HD], qg_ref[...], cos, sin)
        q_ref[:, h * HD:(h + 1) * HD] = q.astype(BF16)
        qt_ref[h * HD:(h + 1) * HD, :] = q.T.astype(BF16)
    k = prep(lin[:, 2 * HD:3 * HD], kg_ref[...], cos, sin)
    k_ref[...] = k.astype(BF16)
    kt_ref[...] = k.T.astype(BF16)
    v = lin[:, 3 * HD:]
    v_ref[...] = v.astype(BF16)
    vt_ref[...] = v.T.astype(BF16)


def project(n_all, w_own, cos, sin, qg, kg):
    toks = n_all.shape[0]
    full = lambda i: (0, 0)
    row = lambda i: (i, 0)
    col = lambda i: (0, i)
    sds = jax.ShapeDtypeStruct
    return pl.pallas_call(
        proj_kernel,
        grid=(toks // BLK,),
        in_specs=[pl.BlockSpec((BLK, n_all.shape[1]), row), pl.BlockSpec(w_own.shape, full),
                  pl.BlockSpec((BLK, HD), row), pl.BlockSpec((BLK, HD), row),
                  pl.BlockSpec((1, HD), full), pl.BlockSpec((1, HD), full)],
        out_specs=[pl.BlockSpec((BLK, 2 * HD), row), pl.BlockSpec((2 * HD, BLK), col),
                   pl.BlockSpec((BLK, HD), row), pl.BlockSpec((HD, BLK), col),
                   pl.BlockSpec((BLK, HD), row), pl.BlockSpec((HD, BLK), col),
                   pl.BlockSpec((BLK, 3 * HD), row)],
        out_shape=[sds((toks, 2 * HD), BF16), sds((2 * HD, toks), BF16), sds((toks, HD), BF16), sds((HD, toks), BF16),
                   sds((toks, HD), BF16), sds((HD, toks), BF16), sds((toks, 3 * HD), F32)],
        compiler_params=pltpu.CompilerParams(vmem_limit_bytes=VMEM_LIMIT),
        cost_estimate=pl.CostEstimate(flops=2 * toks * n_all.shape[1] * 4 * HD, bytes_accessed=30_000_000, transcendentals=0),
        name='proj',
    )(n_all, w_own, cos, sin, qg, kg)


def fwd_kernel(qt_ref, k_ref, vt_ref, do_ref, o_ref, dot_ref, lse_ref, delta_ref, acc, m_s, l_s):
    i = pl.program_id(0)
    scale = HD ** -0.5 * LOG2E
    acc[...] = jnp.zeros_like(acc)
    m_s[...] = jnp.full_like(m_s, MASK_VALUE)
    l_s[...] = jnp.zeros_like(l_s)

    def step(j, masked):
        start = pl.multiple_of(j * BLK, BLK)
        k = k_ref[pl.ds(start, BLK), :]
        vt = vt_ref[:, pl.ds(start, BLK)]
        for h in range(2):
            s = dot_nn(k, qt_ref[h * HD:(h + 1) * HD, :])
            if masked:
                keys = lax.broadcasted_iota(jnp.int32, s.shape, 0)
                queries = lax.broadcasted_iota(jnp.int32, s.shape, 1)
                s = jnp.where(keys <= queries, s, MASK_VALUE)
            m_old = m_s[h:h + 1, :]
            m_new = jnp.maximum(m_old, jnp.max(s, axis=0, keepdims=True))
            p = jnp.exp2((s - m_new) * scale)
            alpha = jnp.exp2((m_old - m_new) * scale)
            m_s[h:h + 1, :] = m_new
            l_s[h:h + 1, :] = l_s[h:h + 1, :] * alpha + jnp.sum(p, axis=0, keepdims=True)
            rows = slice(h * HD, (h + 1) * HD)
            acc[rows, :] = acc[rows, :] * alpha + dot_nn(vt, p.astype(BF16))

    def body(j, carry):
        step(j, False)
        return carry

    lax.fori_loop(0, i, body, 0)
    step(i, True)
    for h in range(2):
        rows = slice(h * HD, (h + 1) * HD)
        l = l_s[h:h + 1, :]
        ot = acc[rows, :] / l
        dot = do_ref[:, rows].astype(F32).T
        dot_ref[rows, :] = dot.astype(BF16)
        delta_ref[h:h + 1, :] = jnp.sum(ot * dot, axis=0, keepdims=True)
        lse_ref[h:h + 1, :] = m_s[h:h + 1, :] * scale + jnp.log2(l)
        o_ref[:, rows] = ot.T.astype(BF16)


def attend(qt, k, vt, do):
    toks = k.shape[0]
    full = lambda i: (0, 0)
    row = lambda i: (i, 0)
    col = lambda i: (0, i)
    sds = jax.ShapeDtypeStruct
    pairs = toks * toks // 2
    return pl.pallas_call(
        fwd_kernel,
        grid=(toks // BLK,),
        in_specs=[pl.BlockSpec((2 * HD, BLK), col), pl.BlockSpec((toks, HD), full), pl.BlockSpec((HD, toks), full),
                  pl.BlockSpec((BLK, 2 * HD), row)],
        out_specs=[pl.BlockSpec((BLK, 2 * HD), row), pl.BlockSpec((2 * HD, BLK), col),
                   pl.BlockSpec((2, BLK), col), pl.BlockSpec((2, BLK), col)],
        out_shape=[sds((toks, 2 * HD), BF16), sds((2 * HD, toks), BF16), sds((2, toks), F32), sds((2, toks), F32)],
        scratch_shapes=[pltpu.VMEM((2 * HD, BLK), F32), pltpu.VMEM((2, BLK), F32), pltpu.VMEM((2, BLK), F32)],
        compiler_params=pltpu.CompilerParams(vmem_limit_bytes=VMEM_LIMIT),
        cost_estimate=pl.CostEstimate(flops=2 * pairs * 4 * HD * 2, bytes_accessed=10_000_000, transcendentals=2 * pairs),
        name='attend',
    )(qt, k, vt, do)


def bwd_kernel(q_ref, qt_ref, do_ref, dot_ref, lse_ref, delta_ref, k_ref, kt_ref, v_ref, lin_ref, cos_ref, sin_ref,
               qg_ref, kg_ref, drot_ref, dlin_ref, dqg_ref, dkg_ref, dqt, dk_s, dv_s):
    j = pl.program_id(0)
    n_blk = pl.num_programs(0)
    scale = HD ** -0.5
    scale2 = scale * LOG2E

    @pl.when(j == 0)
    def _():
        dqt[...] = jnp.zeros_like(dqt)
        dqg_ref[...] = jnp.zeros_like(dqg_ref)
        dkg_ref[...] = jnp.zeros_like(dkg_ref)

    dk_s[...] = jnp.zeros_like(dk_s)
    dv_s[...] = jnp.zeros_like(dv_s)
    k = k_ref[...]
    kt = kt_ref[...]
    v = v_ref[...]

    def step(i, masked):
        start = pl.multiple_of(i * BLK, BLK)
        cols = pl.ds(start, BLK)
        for h in range(2):
            rows = slice(h * HD, (h + 1) * HD)
            s = dot_nn(k, qt_ref[rows, cols])
            p = jnp.exp2(s * scale2 - lse_ref[h:h + 1, cols])
            if masked:
                keys = lax.broadcasted_iota(jnp.int32, s.shape, 0)
                queries = lax.broadcasted_iota(jnp.int32, s.shape, 1)
                p = jnp.where(keys <= queries, p, 0.0)
            dp = dot_nn(v, dot_ref[rows, cols])
            ds = (p * (dp - delta_ref[h:h + 1, cols])).astype(BF16)
            dv_s[...] += dot_nn(p.astype(BF16), do_ref[cols, rows])
            dk_s[...] += dot_nn(ds, q_ref[cols, rows])
            dqt[rows, cols] += dot_nn(kt, ds)

    step(j, True)

    def body(i, carry):
        step(i, False)
        return carry

    lax.fori_loop(j + 1, n_blk, body, 0)

    cos, sin = cos_ref[...], sin_ref[...]
    mine = pl.ds(pl.multiple_of(j * BLK, BLK), BLK)
    for h in range(3):
        rows = slice(h * HD, (h + 1) * HD)
        d_rot = (dqt[rows, mine].T if h < 2 else dk_s[...]) * scale
        d_rot = d_rot.astype(BF16)
        drot_ref[:, rows] = d_rot
        gain = qg_ref[...] if h < 2 else kg_ref[...]
        d_lin, d_gain = prep_back(d_rot.astype(F32), lin_ref[:, rows], gain, cos, sin)
        dlin_ref[:, rows] = d_lin.astype(BF16)
        if h < 2:
            dqg_ref[...] += d_gain
        else:
            dkg_ref[...] += d_gain
    dv = dv_s[...].astype(BF16)
    drot_ref[:, 3 * HD:] = dv
    dlin_ref[:, 3 * HD:] = dv


def attend_back(q, qt, do, dot, lse, delta, k, kt, v, lin, cos, sin, qg, kg):
    toks = k.shape[0]
    full = lambda i: (0, 0)
    row = lambda i: (i, 0)
    col = lambda i: (0, i)
    sds = jax.ShapeDtypeStruct
    pairs = toks * toks // 2
    whole = lambda a: pl.BlockSpec(a.shape, full)
    return pl.pallas_call(
        bwd_kernel,
        grid=(toks // BLK,),
        in_specs=[whole(q), whole(qt), whole(do), whole(dot), whole(lse), whole(delta),
                  pl.BlockSpec((BLK, HD), row), pl.BlockSpec((HD, BLK), col), pl.BlockSpec((BLK, HD), row),
                  pl.BlockSpec((BLK, 3 * HD), row), pl.BlockSpec((BLK, HD), row), pl.BlockSpec((BLK, HD), row),
                  pl.BlockSpec((1, HD), full), pl.BlockSpec((1, HD), full)],
        out_specs=[pl.BlockSpec((BLK, 4 * HD), row), pl.BlockSpec((BLK, 4 * HD), row),
                   pl.BlockSpec((1, HD), full), pl.BlockSpec((1, HD), full)],
        out_shape=[sds((toks, 4 * HD), BF16), sds((toks, 4 * HD), BF16), sds((1, HD), F32), sds((1, HD), F32)],
        scratch_shapes=[pltpu.VMEM((2 * HD, toks), F32), pltpu.VMEM((BLK, HD), F32), pltpu.VMEM((BLK, HD), F32)],
        compiler_params=pltpu.CompilerParams(vmem_limit_bytes=VMEM_LIMIT),
        cost_estimate=pl.CostEstimate(flops=2 * pairs * 10 * HD * 2, bytes_accessed=20_000_000, transcendentals=2 * pairs),
        name='attend_back',
    )(q, qt, do, dot, lse, delta, k, kt, v, lin, cos, sin, qg, kg)


def lin_kernel(n_ref, wq_ref, wk_ref, lin_ref):
    w = jnp.concatenate([wq_ref[...], wk_ref[...]], axis=1)
    lin_ref[0] = dot_nn(n_ref[...], w)


def own_lin(n_own, w_query, w_key):
    toks, dim = n_own.shape
    groups = w_key.shape[1] // HD
    return pl.pallas_call(
        lin_kernel,
        grid=(groups, toks // BLK),
        in_specs=[pl.BlockSpec((BLK, dim), lambda g, t: (t, 0)), pl.BlockSpec((dim, 2 * HD), lambda g, t: (0, g)),
                  pl.BlockSpec((dim, HD), lambda g, t: (0, g))],
        out_specs=pl.BlockSpec((1, BLK, 3 * HD), lambda g, t: (g, t, 0)),
        out_shape=jax.ShapeDtypeStruct((groups, toks, 3 * HD), F32),
        compiler_params=pltpu.CompilerParams(vmem_limit_bytes=VMEM_LIMIT),
        cost_estimate=pl.CostEstimate(flops=2 * toks * dim * 3 * HD * groups, bytes_accessed=60_000_000, transcendentals=0),
        name='own_lin',
    )(n_own, w_query, w_key)


def gradx_kernel(drot_ref, lin_ref, wq_ref, wk_ref, wv_ref, cos_ref, sin_ref, qg_ref, kg_ref, x_ref, gy_ref, ng_ref,
                 gx_ref, dng_ref, acc):
    g = pl.program_id(0)

    @pl.when(g == 0)
    def _():
        acc[...] = jnp.zeros_like(acc)

    cos, sin = cos_ref[...], sin_ref[...]
    parts = []
    for h in range(3):
        rows = slice(h * HD, (h + 1) * HD)
        gain = qg_ref[...] if h < 2 else kg_ref[...]
        d_lin, _ = prep_back(drot_ref[0, :, rows].astype(F32), lin_ref[0, :, rows], gain, cos, sin)
        parts.append(d_lin.astype(BF16))
    parts.append(drot_ref[0, :, 3 * HD:])
    w = jnp.concatenate([wq_ref[...], wk_ref[...], wv_ref[...]], axis=1)
    acc[...] += dot_nt(jnp.concatenate(parts, axis=1), w)

    @pl.when(g == pl.num_programs(0) - 1)
    def _():
        d_n = acc[...].astype(BF16).astype(F32)
        x = x_ref[...].astype(F32)
        r = lax.rsqrt(jnp.mean(x * x, axis=-1, keepdims=True) + EPSILON)
        dng_ref[...] = jnp.sum(d_n * (x * r), axis=0, keepdims=True)
        scaled = d_n * ng_ref[...]
        dot_mean = jnp.mean(scaled * x, axis=-1, keepdims=True)
        gx_ref[...] = (gy_ref[...].astype(F32) + r * scaled - x * (r * r * r * dot_mean)).astype(BF16)


def grad_tokens(drot, lin, seq, w_query, w_key, w_value, cos, sin, qg, kg, x, gy, ng):
    groups, toks, _ = drot.shape
    dim = x.shape[1]
    full = lambda g: (0, 0)
    col = lambda g: (0, g)
    return pl.pallas_call(
        gradx_kernel,
        grid=(groups,),
        in_specs=[pl.BlockSpec((1, toks, 4 * HD), lambda g: (g, 0, 0)), pl.BlockSpec((1, toks, 3 * HD), lambda g: (g, seq, 0)),
                  pl.BlockSpec((dim, 2 * HD), col), pl.BlockSpec((dim, HD), col), pl.BlockSpec((dim, HD), col),
                  pl.BlockSpec((toks, HD), full), pl.BlockSpec((toks, HD), full), pl.BlockSpec((1, HD), full),
                  pl.BlockSpec((1, HD), full), pl.BlockSpec((toks, dim), full), pl.BlockSpec((toks, dim), full),
                  pl.BlockSpec((1, dim), full)],
        out_specs=[pl.BlockSpec((toks, dim), full), pl.BlockSpec((1, dim), full)],
        out_shape=[jax.ShapeDtypeStruct((toks, dim), BF16), jax.ShapeDtypeStruct((1, dim), F32)],
        scratch_shapes=[pltpu.VMEM((toks, dim), F32)],
        compiler_params=pltpu.CompilerParams(vmem_limit_bytes=VMEM_LIMIT),
        cost_estimate=pl.CostEstimate(flops=2 * toks * dim * 4 * HD * groups, bytes_accessed=40_000_000, transcendentals=0),
        name='grad_tokens',
    )(drot, lin, w_query, w_key, w_value, cos, sin, qg, kg, x, gy, ng)


def rope_tables(positions):
    half_dim = HD // 2
    inv_freq = ROPE_THETA ** (-jnp.arange(half_dim, dtype=F32) / half_dim)
    angles = positions.astype(F32)[..., None] * inv_freq
    cos, sin = jnp.cos(angles), jnp.sin(angles)
    return jnp.concatenate([cos, cos], axis=-1), jnp.concatenate([-sin, sin], axis=-1)


def solution(mesh):
    n_dev = mesh.shape[SEQ_AXIS]
    tok_spec = P(None, SEQ_AXIS, None)
    pos_spec = P(None, SEQ_AXIS)

    def swap(x, dist):
        return lax.ppermute(x, SEQ_AXIS, [(d, d ^ dist) for d in range(n_dev)])

    def device_fn(x_in, grad_y, positions, norm_gain, w_query, w_key, w_value, w_out, q_gain, k_gain):
        n_batch, seq_dev, dim = x_in.shape
        me = lax.axis_index(SEQ_AXIS)
        seq_len = seq_dev * n_dev
        ng = norm_gain.astype(F32)[None]
        qg = q_gain.astype(F32)[None]
        kg = k_gain.astype(F32)[None]

        x32 = x_in.astype(F32)
        normed = (x32 * lax.rsqrt(jnp.mean(x32 * x32, axis=-1, keepdims=True) + EPSILON) * ng).astype(BF16)
        n_all = [lax.all_gather(normed[b], SEQ_AXIS, axis=0, tiled=True) for b in range(n_batch)]
        pos_all = lax.all_gather(positions, SEQ_AXIS, axis=1, tiled=True)
        cos_all, sin_all = rope_tables(pos_all)
        cos_own, sin_own = rope_tables(positions)
        own_cols = lambda w, width: lax.dynamic_slice_in_dim(w, me * width, width, axis=1)
        w_own = jnp.concatenate([own_cols(w_query, 2 * HD), own_cols(w_key, HD), own_cols(w_value, HD)], axis=1)
        lin_own = own_lin(normed.reshape(n_batch * seq_dev, dim), w_query, w_key)

        def col_block(a, dev):
            return lax.dynamic_slice_in_dim(a, dev * 2 * HD, 2 * HD, axis=1)

        def row_block(a, dev):
            return lax.dynamic_slice_in_dim(a, dev * seq_dev, seq_dev, axis=0)

        do_all = []
        for b in range(n_batch):
            d_attn = lax.dot_general(grad_y[b], w_out, (((1,), (1,)), ((), ())), preferred_element_type=F32).astype(BF16)
            got = jnp.zeros((seq_len, 2 * HD), BF16)
            for dist in range(n_dev):
                blk = col_block(d_attn, me ^ dist)
                if dist:
                    blk = swap(blk, dist)
                got = lax.dynamic_update_slice_in_dim(got, blk, (me ^ dist) * seq_dev, axis=0)
            do_all.append(got)

        y_out, o_own, saved = [], [], []
        for b in range(n_batch):
            q, qt, k, kt, v, vt, lin = project(n_all[b], w_own, cos_all[b], sin_all[b], qg, kg)
            o, dot, lse, delta = attend(qt, k, vt, do_all[b])
            saved.append((q, qt, do_all[b], dot, lse, delta, k, kt, v, lin))
            got = jnp.zeros((seq_dev, n_dev * 2 * HD), BF16)
            for dist in range(n_dev):
                blk = row_block(o, me ^ dist)
                if dist:
                    blk = swap(blk, dist)
                got = lax.dynamic_update_slice_in_dim(got, blk, (me ^ dist) * 2 * HD, axis=1)
            o_own.append(got)
            y_out.append((x32[b] + dot_nn(got, w_out)).astype(BF16))
        o_cat = jnp.concatenate(o_own, axis=0)
        gy_cat = grad_y.reshape(n_batch * seq_dev, dim)
        grad_w_out = lax.dot_general(o_cat, gy_cat, (((0,), (0,)), ((), ())), preferred_element_type=F32)
        grad_w_out = lax.psum(grad_w_out, SEQ_AXIS)

        grad_x, dng_sum, dqg_sum, dkg_sum, dw_sum = [], 0.0, 0.0, 0.0, 0.0
        for b in range(n_batch):
            drot, dlin, dqg, dkg = attend_back(*saved[b], cos_all[b], sin_all[b], qg, kg)
            dqg_sum, dkg_sum = dqg_sum + dqg, dkg_sum + dkg
            dw_sum = dw_sum + lax.dot_general(n_all[b], dlin, (((0,), (0,)), ((), ())), preferred_element_type=F32)
            got = jnp.zeros((n_dev, seq_dev, 4 * HD), BF16)
            for dist in range(n_dev):
                blk = row_block(drot, me ^ dist)
                if dist:
                    blk = swap(blk, dist)
                got = lax.dynamic_update_slice(got, blk[None], (me ^ dist, 0, 0))
            gx, dng = grad_tokens(got, lin_own, b, w_query, w_key, w_value, cos_own[b], sin_own[b], qg, kg,
                                  x_in[b], grad_y[b], ng)
            grad_x.append(gx)
            dng_sum = dng_sum + dng
        dw_all = lax.all_gather(dw_sum, SEQ_AXIS, axis=0)
        pick = lambda lo, hi: jnp.moveaxis(dw_all[:, :, lo:hi], 0, 1).reshape(dim, -1)
        small = lax.psum((dng_sum[0], dqg_sum[0], dkg_sum[0]), SEQ_AXIS)
        return (jnp.stack(y_out), jnp.stack(grad_x), small[0], pick(0, 2 * HD), pick(2 * HD, 3 * HD), pick(3 * HD, 4 * HD),
                grad_w_out, small[1], small[2])

    in_specs = (tok_spec, tok_spec, pos_spec, P(), P(), P(), P(), P(), P(), P())
    out_specs = (tok_spec, tok_spec, P(), P(), P(), P(), P(), P(), P())
    return jax.shard_map(device_fn, mesh=mesh, in_specs=in_specs, out_specs=out_specs, check_vma=False)
```

```python
import jax
import jax.numpy as jnp
from jax import lax
from jax.experimental import pallas as pl
from jax.experimental.pallas import tpu as pltpu
from jax.sharding import PartitionSpec as P


SEQ_AXIS = 'cp'
ROPE_THETA = 1000000.0
EPSILON = 1e-6
MASK_VALUE = -1e30
LOG2E = 1.4426950408889634
HD = 128
BLK = 512
F32 = jnp.float32
BF16 = jnp.bfloat16
VMEM_LIMIT = 60 * 1024 * 1024


def dot_nn(a, b):
    return lax.dot_general(a, b, (((1,), (0,)), ((), ())), preferred_element_type=F32)


def dot_nt(a, b):
    return lax.dot_general(a, b, (((1,), (1,)), ((), ())), preferred_element_type=F32)


def prep(t, gain, cos, sin):
    r = lax.rsqrt(jnp.mean(t * t, axis=-1, keepdims=True) + EPSILON)
    normed = t * r * gain
    return normed * cos + pltpu.roll(normed, HD // 2, 1) * sin


def prep_back(d_rot, t, gain, cos, sin):
    d_norm = d_rot * cos - pltpu.roll(d_rot, HD // 2, 1) * sin
    r = lax.rsqrt(jnp.mean(t * t, axis=-1, keepdims=True) + EPSILON)
    d_gain = jnp.sum(d_norm * (t * r), axis=0, keepdims=True)
    scaled = d_norm * gain
    dot_mean = jnp.mean(scaled * t, axis=-1, keepdims=True)
    return r * scaled - t * (r * r * r * dot_mean), d_gain


def proj_kernel(n_ref, w_ref, cos_ref, sin_ref, qg_ref, kg_ref, q_ref, qt_ref, k_ref, kt_ref, v_ref, vt_ref, lin_ref):
    sub = BLK // 4
    for part in range(4):
        r = slice(part * sub, (part + 1) * sub)
        lin = dot_nn(n_ref[r, :], w_ref[...])
        lin_ref[r, :] = lin[:, :3 * HD]
        cos, sin = cos_ref[r, :], sin_ref[r, :]
        for h in range(2):
            q = prep(lin[:, h * HD:(h + 1) * HD], qg_ref[...], cos, sin)
            q_ref[r, h * HD:(h + 1) * HD] = q.astype(BF16)
            qt_ref[h * HD:(h + 1) * HD, r] = q.T.astype(BF16)
        k = prep(lin[:, 2 * HD:3 * HD], kg_ref[...], cos, sin)
        k_ref[r, :] = k.astype(BF16)
        kt_ref[:, r] = k.T.astype(BF16)
        v = lin[:, 3 * HD:]
        v_ref[r, :] = v.astype(BF16)
        vt_ref[:, r] = v.T.astype(BF16)


def project(n_all, w_own, cos, sin, qg, kg):
    toks = n_all.shape[0]
    full = lambda i: (0, 0)
    row = lambda i: (i, 0)
    col = lambda i: (0, i)
    sds = jax.ShapeDtypeStruct
    return pl.pallas_call(
        proj_kernel,
        grid=(toks // BLK,),
        in_specs=[pl.BlockSpec((BLK, n_all.shape[1]), row), pl.BlockSpec(w_own.shape, full),
                  pl.BlockSpec((BLK, HD), row), pl.BlockSpec((BLK, HD), row),
                  pl.BlockSpec((1, HD), full), pl.BlockSpec((1, HD), full)],
        out_specs=[pl.BlockSpec((BLK, 2 * HD), row), pl.BlockSpec((2 * HD, BLK), col),
                   pl.BlockSpec((BLK, HD), row), pl.BlockSpec((HD, BLK), col),
                   pl.BlockSpec((BLK, HD), row), pl.BlockSpec((HD, BLK), col),
                   pl.BlockSpec((BLK, 3 * HD), row)],
        out_shape=[sds((toks, 2 * HD), BF16), sds((2 * HD, toks), BF16), sds((toks, HD), BF16), sds((HD, toks), BF16),
                   sds((toks, HD), BF16), sds((HD, toks), BF16), sds((toks, 3 * HD), F32)],
        compiler_params=pltpu.CompilerParams(vmem_limit_bytes=VMEM_LIMIT),
        cost_estimate=pl.CostEstimate(flops=2 * toks * n_all.shape[1] * 4 * HD, bytes_accessed=30_000_000, transcendentals=0),
        name='proj',
    )(n_all, w_own, cos, sin, qg, kg)


def fwd_kernel(qt_ref, k_ref, vt_ref, o_ref, ot_ref, lse_ref, acc, m_s, l_s):
    i = pl.program_id(0)
    scale = HD ** -0.5 * LOG2E
    acc[...] = jnp.zeros_like(acc)
    m_s[...] = jnp.full_like(m_s, MASK_VALUE)
    l_s[...] = jnp.zeros_like(l_s)

    def step(j, masked):
        start = pl.multiple_of(j * BLK, BLK)
        k = k_ref[pl.ds(start, BLK), :]
        vt = vt_ref[:, pl.ds(start, BLK)]
        scores = [dot_nn(k, qt_ref[h * HD:(h + 1) * HD, :]) for h in range(2)]
        for h in range(2):
            s = scores[h]
            if masked:
                keys = lax.broadcasted_iota(jnp.int32, s.shape, 0)
                queries = lax.broadcasted_iota(jnp.int32, s.shape, 1)
                s = jnp.where(keys <= queries, s, MASK_VALUE)
            m_old = m_s[h:h + 1, :]
            m_new = jnp.maximum(m_old, jnp.max(s, axis=0, keepdims=True))
            p = jnp.exp2((s - m_new) * scale)
            alpha = jnp.exp2((m_old - m_new) * scale)
            m_s[h:h + 1, :] = m_new
            l_s[h:h + 1, :] = l_s[h:h + 1, :] * alpha + jnp.sum(p, axis=0, keepdims=True)
            rows = slice(h * HD, (h + 1) * HD)
            acc[rows, :] = acc[rows, :] * alpha + dot_nn(vt, p.astype(BF16))

    def body(j, carry):
        step(j, False)
        return carry

    lax.fori_loop(0, i, body, 0)
    step(i, True)
    for h in range(2):
        rows = slice(h * HD, (h + 1) * HD)
        l = l_s[h:h + 1, :]
        ot = acc[rows, :] / l
        ot_ref[rows, :] = ot
        lse_ref[h:h + 1, :] = m_s[h:h + 1, :] * scale + jnp.log2(l)
        o_ref[:, rows] = ot.T.astype(BF16)


def attend(qt, k, vt):
    toks = k.shape[0]
    full = lambda i: (0, 0)
    row = lambda i: (i, 0)
    col = lambda i: (0, i)
    sds = jax.ShapeDtypeStruct
    pairs = toks * toks // 2
    return pl.pallas_call(
        fwd_kernel,
        grid=(toks // BLK,),
        in_specs=[pl.BlockSpec((2 * HD, BLK), col), pl.BlockSpec((toks, HD), full), pl.BlockSpec((HD, toks), full)],
        out_specs=[pl.BlockSpec((BLK, 2 * HD), row), pl.BlockSpec((2 * HD, BLK), col), pl.BlockSpec((2, BLK), col)],
        out_shape=[sds((toks, 2 * HD), BF16), sds((2 * HD, toks), F32), sds((2, toks), F32)],
        scratch_shapes=[pltpu.VMEM((2 * HD, BLK), F32), pltpu.VMEM((2, BLK), F32), pltpu.VMEM((2, BLK), F32)],
        compiler_params=pltpu.CompilerParams(vmem_limit_bytes=VMEM_LIMIT),
        cost_estimate=pl.CostEstimate(flops=2 * pairs * 4 * HD * 2, bytes_accessed=10_000_000, transcendentals=2 * pairs),
        name='attend',
    )(qt, k, vt)


def bwd_kernel(q_ref, qt_ref, do_ref, ot_ref, lse_ref, k_ref, kt_ref, v_ref, lin_ref, cos_ref, sin_ref,
               qg_ref, kg_ref, drot_ref, dlin_ref, dqg_ref, dkg_ref, dqt, dk_s, dv_s, dot_ref, delta_ref):
    j = pl.program_id(0)
    n_blk = pl.num_programs(0)
    scale = HD ** -0.5
    scale2 = scale * LOG2E

    @pl.when(j == 0)
    def _():
        dqt[...] = jnp.zeros_like(dqt)
        dqg_ref[...] = jnp.zeros_like(dqg_ref)
        dkg_ref[...] = jnp.zeros_like(dkg_ref)

        def turn(i, carry):
            part = pl.ds(pl.multiple_of(i * BLK, BLK), BLK)
            for h in range(2):
                rows = slice(h * HD, (h + 1) * HD)
                dot = do_ref[part, rows].astype(F32).T
                dot_ref[rows, part] = dot.astype(BF16)
                delta_ref[h:h + 1, part] = jnp.sum(ot_ref[rows, part] * dot, axis=0, keepdims=True)
            return carry

        lax.fori_loop(0, n_blk, turn, 0)

    dk_s[...] = jnp.zeros_like(dk_s)
    dv_s[...] = jnp.zeros_like(dv_s)
    k = k_ref[...]
    kt = kt_ref[...]
    v = v_ref[...]

    def step(i, masked):
        start = pl.multiple_of(i * BLK, BLK)
        cols = pl.ds(start, BLK)
        for h in range(2):
            rows = slice(h * HD, (h + 1) * HD)
            s = dot_nn(k, qt_ref[rows, cols])
            p = jnp.exp2(s * scale2 - lse_ref[h:h + 1, cols])
            if masked:
                keys = lax.broadcasted_iota(jnp.int32, s.shape, 0)
                queries = lax.broadcasted_iota(jnp.int32, s.shape, 1)
                p = jnp.where(keys <= queries, p, 0.0)
            dp = dot_nn(v, dot_ref[rows, cols])
            ds = (p * (dp - delta_ref[h:h + 1, cols])).astype(BF16)
            dv_s[...] += dot_nn(p.astype(BF16), do_ref[cols, rows])
            dk_s[...] += dot_nn(ds, q_ref[cols, rows])
            dqt[rows, cols] += dot_nn(kt, ds)

    step(j, True)

    def body(i, carry):
        step(i, False)
        return carry

    lax.fori_loop(j + 1, n_blk, body, 0)

    cos, sin = cos_ref[...], sin_ref[...]
    mine = pl.ds(pl.multiple_of(j * BLK, BLK), BLK)
    for h in range(3):
        rows = slice(h * HD, (h + 1) * HD)
        d_rot = (dqt[rows, mine].T if h < 2 else dk_s[...]) * scale
        d_rot = d_rot.astype(BF16)
        drot_ref[:, rows] = d_rot
        gain = qg_ref[...] if h < 2 else kg_ref[...]
        d_lin, d_gain = prep_back(d_rot.astype(F32), lin_ref[:, rows], gain, cos, sin)
        dlin_ref[:, rows] = d_lin.astype(BF16)
        if h < 2:
            dqg_ref[...] += d_gain
        else:
            dkg_ref[...] += d_gain
    dv = dv_s[...].astype(BF16)
    drot_ref[:, 3 * HD:] = dv
    dlin_ref[:, 3 * HD:] = dv


def attend_back(q, qt, do, seq, ot, lse, k, kt, v, lin, cos, sin, qg, kg):
    toks = k.shape[0]
    full = lambda i: (0, 0)
    row = lambda i: (i, 0)
    col = lambda i: (0, i)
    sds = jax.ShapeDtypeStruct
    pairs = toks * toks // 2
    whole = lambda a: pl.BlockSpec(a.shape, full)
    return pl.pallas_call(
        bwd_kernel,
        grid=(toks // BLK,),
        in_specs=[whole(q), whole(qt), pl.BlockSpec((None, toks, 2 * HD), lambda i: (seq, 0, 0)), whole(ot), whole(lse),
                  pl.BlockSpec((BLK, HD), row), pl.BlockSpec((HD, BLK), col), pl.BlockSpec((BLK, HD), row),
                  pl.BlockSpec((BLK, 3 * HD), row), pl.BlockSpec((BLK, HD), row), pl.BlockSpec((BLK, HD), row),
                  pl.BlockSpec((1, HD), full), pl.BlockSpec((1, HD), full)],
        out_specs=[pl.BlockSpec((BLK, 4 * HD), row), pl.BlockSpec((BLK, 4 * HD), row),
                   pl.BlockSpec((1, HD), full), pl.BlockSpec((1, HD), full)],
        out_shape=[sds((toks, 4 * HD), BF16), sds((toks, 4 * HD), BF16), sds((1, HD), F32), sds((1, HD), F32)],
        scratch_shapes=[pltpu.VMEM((2 * HD, toks), F32), pltpu.VMEM((BLK, HD), F32), pltpu.VMEM((BLK, HD), F32),
                        pltpu.VMEM((2 * HD, toks), BF16), pltpu.VMEM((2, toks), F32)],
        compiler_params=pltpu.CompilerParams(vmem_limit_bytes=VMEM_LIMIT),
        cost_estimate=pl.CostEstimate(flops=2 * pairs * 10 * HD * 2, bytes_accessed=20_000_000, transcendentals=2 * pairs),
        name='attend_back',
    )(q, qt, do, ot, lse, k, kt, v, lin, cos, sin, qg, kg)


def lin_kernel(n_ref, wq_ref, wk_ref, lin_ref):
    w = jnp.concatenate([wq_ref[...], wk_ref[...]], axis=1)
    for t in range(n_ref.shape[0] // BLK):
        rows = slice(t * BLK, (t + 1) * BLK)
        lin_ref[0, rows, :] = dot_nn(n_ref[rows, :], w)


def own_lin(n_own, w_query, w_key):
    toks, dim = n_own.shape
    groups = w_key.shape[1] // HD
    return pl.pallas_call(
        lin_kernel,
        grid=(groups,),
        in_specs=[pl.BlockSpec((toks, dim), lambda g: (0, 0)), pl.BlockSpec((dim, 2 * HD), lambda g: (0, g)),
                  pl.BlockSpec((dim, HD), lambda g: (0, g))],
        out_specs=pl.BlockSpec((1, toks, 3 * HD), lambda g: (g, 0, 0)),
        out_shape=jax.ShapeDtypeStruct((groups, toks, 3 * HD), F32),
        compiler_params=pltpu.CompilerParams(vmem_limit_bytes=VMEM_LIMIT),
        cost_estimate=pl.CostEstimate(flops=2 * toks * dim * 3 * HD * groups, bytes_accessed=60_000_000, transcendentals=0),
        name='own_lin',
    )(n_own, w_query, w_key)


def gradx_kernel(drot_ref, lin_ref, wq_ref, wk_ref, wv_ref, cos_ref, sin_ref, qg_ref, kg_ref, x_ref, gy_ref, ng_ref,
                 *rest):
    gx_ref, dng_ref, acc = rest[-3:]
    g = pl.program_id(0)

    @pl.when(g == 0)
    def _():
        acc[...] = jnp.zeros_like(acc)

    cos, sin = cos_ref[...], sin_ref[...]
    parts = []
    for h in range(3):
        rows = slice(h * HD, (h + 1) * HD)
        gain = qg_ref[...] if h < 2 else kg_ref[...]
        d_lin, _ = prep_back(drot_ref[0, :, rows].astype(F32), lin_ref[0, :, rows], gain, cos, sin)
        parts.append(d_lin.astype(BF16))
    parts.append(drot_ref[0, :, 3 * HD:])
    w = jnp.concatenate([wq_ref[...], wk_ref[...], wv_ref[...]], axis=1)
    acc[...] += dot_nt(jnp.concatenate(parts, axis=1), w)

    @pl.when(g == pl.num_programs(0) - 1)
    def _():
        d_n = acc[...].astype(BF16).astype(F32)
        x = x_ref[0].astype(F32)
        r = lax.rsqrt(jnp.mean(x * x, axis=-1, keepdims=True) + EPSILON)
        dng_ref[...] = jnp.sum(d_n * (x * r), axis=0, keepdims=True)
        scaled = d_n * ng_ref[...]
        dot_mean = jnp.mean(scaled * x, axis=-1, keepdims=True)
        gx_ref[0] = (gy_ref[0].astype(F32) + r * scaled - x * (r * r * r * dot_mean)).astype(BF16)


def grad_tokens(drot, lin, seq, w_query, w_key, w_value, cos, sin, qg, kg, x, gy, ng, so_far):
    groups, toks, _ = drot.shape
    dim = x.shape[2]
    own = pl.BlockSpec((1, toks, dim), lambda g: (seq, 0, 0))
    extra = () if so_far is None else (so_far,)
    full = lambda g: (0, 0)
    col = lambda g: (0, g)
    return pl.pallas_call(
        gradx_kernel,
        grid=(groups,),
        in_specs=[pl.BlockSpec((1, toks, 4 * HD), lambda g: (g, 0, 0)), pl.BlockSpec((1, toks, 3 * HD), lambda g: (g, seq, 0)),
                  pl.BlockSpec((dim, 2 * HD), col), pl.BlockSpec((dim, HD), col), pl.BlockSpec((dim, HD), col),
                  pl.BlockSpec((toks, HD), full), pl.BlockSpec((toks, HD), full), pl.BlockSpec((1, HD), full),
                  pl.BlockSpec((1, HD), full), own, own,
                  pl.BlockSpec((1, dim), full)] + [pl.BlockSpec(memory_space=pl.ANY)] * len(extra),
        out_specs=[own, pl.BlockSpec((1, dim), full)],
        out_shape=[jax.ShapeDtypeStruct(x.shape, BF16), jax.ShapeDtypeStruct((1, dim), F32)],
        input_output_aliases={12: 0} if extra else {},
        scratch_shapes=[pltpu.VMEM((toks, dim), F32)],
        compiler_params=pltpu.CompilerParams(vmem_limit_bytes=VMEM_LIMIT),
        cost_estimate=pl.CostEstimate(flops=2 * toks * dim * 4 * HD * groups, bytes_accessed=40_000_000, transcendentals=0),
        name='grad_tokens',
    )(drot, lin, w_query, w_key, w_value, cos, sin, qg, kg, x, gy, ng, *extra)


def alloc(shape, dtype):
    return pl.pallas_call(lambda out_ref: None, out_specs=pl.BlockSpec(memory_space=pl.ANY),
                          out_shape=jax.ShapeDtypeStruct(shape, dtype), name='alloc')()


def rope_tables(positions):
    half_dim = HD // 2
    inv_freq = ROPE_THETA ** (-jnp.arange(half_dim, dtype=F32) / half_dim)
    angles = positions.astype(F32)[..., None] * inv_freq
    cos, sin = jnp.cos(angles), jnp.sin(angles)
    return jnp.concatenate([cos, cos], axis=-1), jnp.concatenate([-sin, sin], axis=-1)


def solution(mesh):
    n_dev = mesh.shape[SEQ_AXIS]
    tok_spec = P(None, SEQ_AXIS, None)
    pos_spec = P(None, SEQ_AXIS)

    def swap(x, dist):
        return lax.ppermute(x, SEQ_AXIS, [(d, d ^ dist) for d in range(n_dev)])

    def device_fn(x_in, grad_y, positions, norm_gain, w_query, w_key, w_value, w_out, q_gain, k_gain):
        n_batch, seq_dev, dim = x_in.shape
        me = lax.axis_index(SEQ_AXIS)
        seq_len = seq_dev * n_dev
        ng = norm_gain.astype(F32)[None]
        qg = q_gain.astype(F32)[None]
        kg = k_gain.astype(F32)[None]

        x32 = x_in.astype(F32)
        normed = (x32 * lax.rsqrt(jnp.mean(x32 * x32, axis=-1, keepdims=True) + EPSILON) * ng).astype(BF16)

        def after(values, *waits):
            return lax.optimization_barrier((values, waits))[0]

        pos_all = alloc((n_batch, seq_len), jnp.int32)
        for dist in range(n_dev):
            pos_all = lax.dynamic_update_slice(pos_all, swap(positions, dist) if dist else positions, (0, (me ^ dist) * seq_dev))
        normed = after(normed, pos_all)
        n_all = [lax.all_gather(normed[b], SEQ_AXIS, axis=0, tiled=True) for b in range(n_batch)]
        cos_all, sin_all = rope_tables(pos_all)
        cos_own, sin_own = rope_tables(positions)
        own_cols = lambda w, width: lax.dynamic_slice_in_dim(w, me * width, width, axis=1)
        w_own = jnp.concatenate([own_cols(w_query, 2 * HD), own_cols(w_key, HD), own_cols(w_value, HD)], axis=1)

        def col_block(a, dev):
            return lax.dynamic_slice_in_dim(a, dev * 2 * HD, 2 * HD, axis=1)

        def row_block(a, dev):
            return lax.dynamic_slice_in_dim(a, dev * seq_dev, seq_dev, axis=0)

        def exchange(src, cut, put, got, window):
            here, src = lax.optimization_barrier((me, src))
            blocks = [cut(src, here ^ dist) for dist in range(1, n_dev)]
            came = [swap(blk, dist) for dist, blk in enumerate(blocks, 1)]
            came = after([cut(src, here)] + came, window)
            for dist in range(n_dev):
                got = put(got, came[dist], me ^ dist)
            return got

        gy_cat = grad_y.reshape(n_batch * seq_dev, dim)
        d_attn = dot_nt(gy_cat, w_out).astype(BF16)
        n_first, cos_all, sin_all, _ = lax.optimization_barrier((n_all[0], cos_all, sin_all, d_attn))
        n_in = [n_first, n_all[1], n_all[2]]
        saved, outs = [], []
        for b in range(n_batch):
            q, qt, k, kt, v, vt, lin = project(n_in[b], w_own, cos_all[b], sin_all[b], qg, kg)
            o, ot, lse = attend(qt, k, vt)
            saved.append((ot, lse, q, qt, k, kt, v, lin))
            outs.append(o)
            if b == 0:
                lin_own = own_lin(after(normed, lse).reshape(n_batch * seq_dev, dim), w_query, w_key)
                n_in[1] = after(n_in[1], lin_own)

        put_do = lambda got, blk, dev: lax.dynamic_update_slice(got, blk.reshape(n_batch, seq_dev, 2 * HD), (0, dev * seq_dev, 0))
        do_src = after(d_attn, saved[1][1])
        do_all = exchange(do_src, col_block, put_do, alloc((n_batch, seq_len, 2 * HD), BF16), saved[2][1])

        def take_o(b, o_cat, window):
            put = lambda got, blk, dev: lax.dynamic_update_slice(got, blk, (b * seq_dev, dev * 2 * HD))
            return exchange(outs[b], row_block, put, o_cat, window)

        def take_drot(drot, window):
            put = lambda got, blk, dev: lax.dynamic_update_slice(got, blk[None], (dev, 0, 0))
            return exchange(drot, row_block, put, alloc((n_dev, seq_dev, 4 * HD), BF16), window)

        def back(b, waits):
            ot, lse, q, qt, k, kt, v, lin = saved[b]
            q = after(q, waits)
            drot, dlin, dqg, dkg = attend_back(q, qt, do_all, b, ot, lse, k, kt, v, lin, cos_all[b], sin_all[b], qg, kg)
            dw = lax.dot_general(n_all[b], dlin, (((0,), (0,)), ((), ())), preferred_element_type=F32)
            return drot, dqg, dkg, dw

        def to_tokens(b, got, so_far):
            return grad_tokens(got, lin_own, b, w_query, w_key, w_value, cos_own[b], sin_own[b], qg, kg,
                               x_in, grad_y, ng, so_far)

        o_cat = alloc((n_batch * seq_dev, n_dev * 2 * HD), BF16)
        o_cat = take_o(0, o_cat, saved[2][1])
        drot0, dqg0, dkg0, dw0 = back(0, ())
        o_cat = take_o(1, o_cat, drot0)
        o_cat = take_o(2, o_cat, drot0)
        part = lax.dot_general(o_cat, gy_cat, (((0,), (0,)), ((), ())), preferred_element_type=F32)
        grad_w_out = lax.psum_scatter(part, SEQ_AXIS, scatter_dimension=0, tiled=True)
        drot1, dqg1, dkg1, dw1 = back(1, (part, dw0))
        dw01 = dw0 + dw1
        y_out = (x32.reshape(n_batch * seq_dev, dim) + dot_nn(after(o_cat, dw01), w_out)).astype(BF16).reshape(x_in.shape)
        grad_w_out = lax.all_gather(after(grad_w_out, (y_out, dw01)), SEQ_AXIS, axis=0, tiled=True)
        got0 = take_drot(drot0, drot1)
        drot2, dqg2, dkg2, dw2 = back(2, (dw01, y_out))
        dw_sum = dw01 + dw2
        got1 = take_drot(drot1, drot2)
        grad_x, dng0 = to_tokens(0, after(got0, dw_sum), None)
        grad_x, dng1 = to_tokens(1, got1, grad_x)
        grad_x, dng2 = to_tokens(2, take_drot(drot2, grad_x), grad_x)
        dng_sum, dqg_sum, dkg_sum = dng0 + dng1 + dng2, dqg0 + dqg1 + dqg2, dkg0 + dkg1 + dkg2

        def gather_cols(own):
            return jnp.moveaxis(lax.all_gather(own, SEQ_AXIS, axis=0), 0, 1).reshape(dim, -1)

        dw_sum, grad_w_out = lax.optimization_barrier((dw_sum, grad_w_out))
        grad_w_query = gather_cols(dw_sum[:, :2 * HD])
        dw_kv = lax.all_gather(after(dw_sum[:, 2 * HD:], dng0), SEQ_AXIS, axis=0)
        grad_w_key = jnp.moveaxis(dw_kv[:, :, :HD], 0, 1).reshape(dim, -1)
        grad_w_value = jnp.moveaxis(dw_kv[:, :, HD:], 0, 1).reshape(dim, -1)

        small = jnp.concatenate([dng_sum, dqg_sum, dkg_sum], axis=1)
        for dist in (1, 2, 4):
            small = small + swap(small, dist)
        small = small[0]
        return (y_out, grad_x, small[:dim], grad_w_query, grad_w_key, grad_w_value, grad_w_out,
                small[dim:dim + HD], small[dim + HD:])

    in_specs = (tok_spec, tok_spec, pos_spec, P(), P(), P(), P(), P(), P(), P())
    out_specs = (tok_spec, tok_spec, P(), P(), P(), P(), P(), P(), P())
    return jax.shard_map(device_fn, mesh=mesh, in_specs=in_specs, out_specs=out_specs, check_vma=False)
```

```python
import jax
import jax.numpy as jnp
from jax import lax
from jax.experimental import pallas as pl
from jax.experimental.pallas import tpu as pltpu
from jax.sharding import PartitionSpec as P


SEQ_AXIS = 'cp'
ROPE_THETA = 1000000.0
EPSILON = 1e-6
MASK_VALUE = -1e30
LOG2E = 1.4426950408889634
HD = 128
BLK = 512
F32 = jnp.float32
BF16 = jnp.bfloat16
VMEM_LIMIT = 60 * 1024 * 1024


def dot_nn(a, b):
    return lax.dot_general(a, b, (((1,), (0,)), ((), ())), preferred_element_type=F32)


def dot_nt(a, b):
    return lax.dot_general(a, b, (((1,), (1,)), ((), ())), preferred_element_type=F32)


def prep(t, gain, cos, sin):
    r = lax.rsqrt(jnp.mean(t * t, axis=-1, keepdims=True) + EPSILON)
    normed = t * r * gain
    return normed * cos + pltpu.roll(normed, HD // 2, 1) * sin


def prep_back(d_rot, t, gain, cos, sin):
    d_norm = d_rot * cos - pltpu.roll(d_rot, HD // 2, 1) * sin
    r = lax.rsqrt(jnp.mean(t * t, axis=-1, keepdims=True) + EPSILON)
    d_gain = jnp.sum(d_norm * (t * r), axis=0, keepdims=True)
    scaled = d_norm * gain
    dot_mean = jnp.mean(scaled * t, axis=-1, keepdims=True)
    return r * scaled - t * (r * r * r * dot_mean), d_gain


def proj_kernel(n_ref, w_ref, cos_ref, sin_ref, qg_ref, kg_ref, q_ref, qt_ref, k_ref, kt_ref, v_ref, vt_ref, lin_ref):
    sub = BLK // 4
    for part in range(4):
        r = slice(part * sub, (part + 1) * sub)
        lin = dot_nn(n_ref[r, :], w_ref[...])
        lin_ref[r, :] = lin[:, :3 * HD]
        cos, sin = cos_ref[r, :], sin_ref[r, :]
        for h in range(2):
            q = prep(lin[:, h * HD:(h + 1) * HD], qg_ref[...], cos, sin)
            q_ref[r, h * HD:(h + 1) * HD] = q.astype(BF16)
            qt_ref[h * HD:(h + 1) * HD, r] = q.T.astype(BF16)
        k = prep(lin[:, 2 * HD:3 * HD], kg_ref[...], cos, sin)
        k_ref[r, :] = k.astype(BF16)
        kt_ref[:, r] = k.T.astype(BF16)
        v = lin[:, 3 * HD:]
        v_ref[r, :] = v.astype(BF16)
        vt_ref[:, r] = v.T.astype(BF16)


def project(n_all, w_own, cos, sin, qg, kg):
    toks = n_all.shape[0]
    full = lambda i: (0, 0)
    row = lambda i: (i, 0)
    col = lambda i: (0, i)
    sds = jax.ShapeDtypeStruct
    return pl.pallas_call(
        proj_kernel,
        grid=(toks // BLK,),
        in_specs=[pl.BlockSpec((BLK, n_all.shape[1]), row), pl.BlockSpec(w_own.shape, full),
                  pl.BlockSpec((BLK, HD), row), pl.BlockSpec((BLK, HD), row),
                  pl.BlockSpec((1, HD), full), pl.BlockSpec((1, HD), full)],
        out_specs=[pl.BlockSpec((BLK, 2 * HD), row), pl.BlockSpec((2 * HD, BLK), col),
                   pl.BlockSpec((BLK, HD), row), pl.BlockSpec((HD, BLK), col),
                   pl.BlockSpec((BLK, HD), row), pl.BlockSpec((HD, BLK), col),
                   pl.BlockSpec((BLK, 3 * HD), row)],
        out_shape=[sds((toks, 2 * HD), BF16), sds((2 * HD, toks), BF16), sds((toks, HD), BF16), sds((HD, toks), BF16),
                   sds((toks, HD), BF16), sds((HD, toks), BF16), sds((toks, 3 * HD), F32)],
        compiler_params=pltpu.CompilerParams(vmem_limit_bytes=VMEM_LIMIT),
        cost_estimate=pl.CostEstimate(flops=2 * toks * n_all.shape[1] * 4 * HD, bytes_accessed=30_000_000, transcendentals=0),
        name='proj',
    )(n_all, w_own, cos, sin, qg, kg)


def fwd_kernel(qt_ref, k_ref, vt_ref, o_ref, ot_ref, lse_ref, acc, m_s, l_s):
    i = pl.program_id(0)
    scale = HD ** -0.5 * LOG2E
    acc[...] = jnp.zeros_like(acc)
    m_s[...] = jnp.full_like(m_s, MASK_VALUE)
    l_s[...] = jnp.zeros_like(l_s)

    def step(j, masked):
        start = pl.multiple_of(j * BLK, BLK)
        k = k_ref[pl.ds(start, BLK), :]
        vt = vt_ref[:, pl.ds(start, BLK)]
        scores = [dot_nn(k, qt_ref[h * HD:(h + 1) * HD, :]) for h in range(2)]
        for h in range(2):
            s = scores[h]
            if masked:
                keys = lax.broadcasted_iota(jnp.int32, s.shape, 0)
                queries = lax.broadcasted_iota(jnp.int32, s.shape, 1)
                s = jnp.where(keys <= queries, s, MASK_VALUE)
            m_old = m_s[h:h + 1, :]
            m_new = jnp.maximum(m_old, jnp.max(s, axis=0, keepdims=True))
            p = jnp.exp2((s - m_new) * scale)
            alpha = jnp.exp2((m_old - m_new) * scale)
            m_s[h:h + 1, :] = m_new
            l_s[h:h + 1, :] = l_s[h:h + 1, :] * alpha + jnp.sum(p, axis=0, keepdims=True)
            rows = slice(h * HD, (h + 1) * HD)
            acc[rows, :] = acc[rows, :] * alpha + dot_nn(vt, p.astype(BF16))

    def body(j, carry):
        step(j, False)
        return carry

    lax.fori_loop(0, i, body, 0)
    step(i, True)
    for h in range(2):
        rows = slice(h * HD, (h + 1) * HD)
        l = l_s[h:h + 1, :]
        ot = acc[rows, :] / l
        ot_ref[rows, :] = ot
        lse_ref[h:h + 1, :] = m_s[h:h + 1, :] * scale + jnp.log2(l)
        o_ref[:, rows] = ot.T.astype(BF16)


def attend(qt, k, vt):
    toks = k.shape[0]
    full = lambda i: (0, 0)
    row = lambda i: (i, 0)
    col = lambda i: (0, i)
    sds = jax.ShapeDtypeStruct
    pairs = toks * toks // 2
    return pl.pallas_call(
        fwd_kernel,
        grid=(toks // BLK,),
        in_specs=[pl.BlockSpec((2 * HD, BLK), col), pl.BlockSpec((toks, HD), full), pl.BlockSpec((HD, toks), full)],
        out_specs=[pl.BlockSpec((BLK, 2 * HD), row), pl.BlockSpec((2 * HD, BLK), col), pl.BlockSpec((2, BLK), col)],
        out_shape=[sds((toks, 2 * HD), BF16), sds((2 * HD, toks), F32), sds((2, toks), F32)],
        scratch_shapes=[pltpu.VMEM((2 * HD, BLK), F32), pltpu.VMEM((2, BLK), F32), pltpu.VMEM((2, BLK), F32)],
        compiler_params=pltpu.CompilerParams(vmem_limit_bytes=VMEM_LIMIT),
        cost_estimate=pl.CostEstimate(flops=2 * pairs * 4 * HD * 2, bytes_accessed=10_000_000, transcendentals=2 * pairs),
        name='attend',
    )(qt, k, vt)


def bwd_kernel(q_ref, qt_ref, do_ref, ot_ref, lse_ref, k_ref, kt_ref, v_ref, lin_ref, cos_ref, sin_ref,
               qg_ref, kg_ref, drot_ref, dlin_ref, dqg_ref, dkg_ref, dqt, dk_s, dv_s, dot_ref, delta_ref):
    j = pl.program_id(0)
    n_blk = pl.num_programs(0)
    scale = HD ** -0.5
    scale2 = scale * LOG2E

    @pl.when(j == 0)
    def _():
        dqt[...] = jnp.zeros_like(dqt)
        dqg_ref[...] = jnp.zeros_like(dqg_ref)
        dkg_ref[...] = jnp.zeros_like(dkg_ref)

        def turn(i, carry):
            part = pl.ds(pl.multiple_of(i * BLK, BLK), BLK)
            for h in range(2):
                rows = slice(h * HD, (h + 1) * HD)
                dot = do_ref[part, rows].astype(F32).T
                dot_ref[rows, part] = dot.astype(BF16)
                delta_ref[h:h + 1, part] = jnp.sum(ot_ref[rows, part] * dot, axis=0, keepdims=True)
            return carry

        lax.fori_loop(0, n_blk, turn, 0)

    dk_s[...] = jnp.zeros_like(dk_s)
    dv_s[...] = jnp.zeros_like(dv_s)
    k = k_ref[...]
    kt = kt_ref[...]
    v = v_ref[...]

    def step(i, masked):
        start = pl.multiple_of(i * BLK, BLK)
        cols = pl.ds(start, BLK)
        for h in range(2):
            rows = slice(h * HD, (h + 1) * HD)
            s = dot_nn(k, qt_ref[rows, cols])
            p = jnp.exp2(s * scale2 - lse_ref[h:h + 1, cols])
            if masked:
                keys = lax.broadcasted_iota(jnp.int32, s.shape, 0)
                queries = lax.broadcasted_iota(jnp.int32, s.shape, 1)
                p = jnp.where(keys <= queries, p, 0.0)
            dp = dot_nn(v, dot_ref[rows, cols])
            ds = (p * (dp - delta_ref[h:h + 1, cols])).astype(BF16)
            dv_s[...] += dot_nn(p.astype(BF16), do_ref[cols, rows])
            dk_s[...] += dot_nn(ds, q_ref[cols, rows])
            dqt[rows, cols] += dot_nn(kt, ds)

    step(j, True)

    def body(i, carry):
        step(i, False)
        return carry

    lax.fori_loop(j + 1, n_blk, body, 0)

    cos, sin = cos_ref[...], sin_ref[...]
    mine = pl.ds(pl.multiple_of(j * BLK, BLK), BLK)
    for h in range(3):
        rows = slice(h * HD, (h + 1) * HD)
        d_rot = (dqt[rows, mine].T if h < 2 else dk_s[...]) * scale
        d_rot = d_rot.astype(BF16)
        drot_ref[:, rows] = d_rot
        gain = qg_ref[...] if h < 2 else kg_ref[...]
        d_lin, d_gain = prep_back(d_rot.astype(F32), lin_ref[:, rows], gain, cos, sin)
        dlin_ref[:, rows] = d_lin.astype(BF16)
        if h < 2:
            dqg_ref[...] += d_gain
        else:
            dkg_ref[...] += d_gain
    dv = dv_s[...].astype(BF16)
    drot_ref[:, 3 * HD:] = dv
    dlin_ref[:, 3 * HD:] = dv


def attend_back(q, qt, do, seq, ot, lse, k, kt, v, lin, cos, sin, qg, kg):
    toks = k.shape[0]
    full = lambda i: (0, 0)
    row = lambda i: (i, 0)
    col = lambda i: (0, i)
    sds = jax.ShapeDtypeStruct
    pairs = toks * toks // 2
    whole = lambda a: pl.BlockSpec(a.shape, full)
    return pl.pallas_call(
        bwd_kernel,
        grid=(toks // BLK,),
        in_specs=[whole(q), whole(qt), pl.BlockSpec((None, toks, 2 * HD), lambda i: (seq, 0, 0)), whole(ot), whole(lse),
                  pl.BlockSpec((BLK, HD), row), pl.BlockSpec((HD, BLK), col), pl.BlockSpec((BLK, HD), row),
                  pl.BlockSpec((BLK, 3 * HD), row), pl.BlockSpec((BLK, HD), row), pl.BlockSpec((BLK, HD), row),
                  pl.BlockSpec((1, HD), full), pl.BlockSpec((1, HD), full)],
        out_specs=[pl.BlockSpec((BLK, 4 * HD), row), pl.BlockSpec((BLK, 4 * HD), row),
                   pl.BlockSpec((1, HD), full), pl.BlockSpec((1, HD), full)],
        out_shape=[sds((toks, 4 * HD), BF16), sds((toks, 4 * HD), BF16), sds((1, HD), F32), sds((1, HD), F32)],
        scratch_shapes=[pltpu.VMEM((2 * HD, toks), F32), pltpu.VMEM((BLK, HD), F32), pltpu.VMEM((BLK, HD), F32),
                        pltpu.VMEM((2 * HD, toks), BF16), pltpu.VMEM((2, toks), F32)],
        compiler_params=pltpu.CompilerParams(vmem_limit_bytes=VMEM_LIMIT),
        cost_estimate=pl.CostEstimate(flops=2 * pairs * 10 * HD * 2, bytes_accessed=20_000_000, transcendentals=2 * pairs),
        name='attend_back',
    )(q, qt, do, ot, lse, k, kt, v, lin, cos, sin, qg, kg)


def lin_kernel(n_ref, wq_ref, wk_ref, lin_ref):
    w = jnp.concatenate([wq_ref[...], wk_ref[...]], axis=1)
    for t in range(n_ref.shape[0] // BLK):
        rows = slice(t * BLK, (t + 1) * BLK)
        lin_ref[0, rows, :] = dot_nn(n_ref[rows, :], w)


def own_lin(n_own, w_query, w_key):
    toks, dim = n_own.shape
    groups = w_key.shape[1] // HD
    return pl.pallas_call(
        lin_kernel,
        grid=(groups,),
        in_specs=[pl.BlockSpec((toks, dim), lambda g: (0, 0)), pl.BlockSpec((dim, 2 * HD), lambda g: (0, g)),
                  pl.BlockSpec((dim, HD), lambda g: (0, g))],
        out_specs=pl.BlockSpec((1, toks, 3 * HD), lambda g: (g, 0, 0)),
        out_shape=jax.ShapeDtypeStruct((groups, toks, 3 * HD), F32),
        compiler_params=pltpu.CompilerParams(vmem_limit_bytes=VMEM_LIMIT),
        cost_estimate=pl.CostEstimate(flops=2 * toks * dim * 3 * HD * groups, bytes_accessed=60_000_000, transcendentals=0),
        name='own_lin',
    )(n_own, w_query, w_key)


def gradx_kernel(drot_ref, lin_ref, wq_ref, wk_ref, wv_ref, cos_ref, sin_ref, qg_ref, kg_ref, x_ref, gy_ref, ng_ref,
                 *rest):
    gx_ref, dng_ref, acc = rest[-3:]
    g = pl.program_id(0)

    @pl.when(g == 0)
    def _():
        acc[...] = jnp.zeros_like(acc)

    cos, sin = cos_ref[...], sin_ref[...]
    parts = []
    for h in range(3):
        rows = slice(h * HD, (h + 1) * HD)
        gain = qg_ref[...] if h < 2 else kg_ref[...]
        d_lin, _ = prep_back(drot_ref[0, :, rows].astype(F32), lin_ref[0, :, rows], gain, cos, sin)
        parts.append(d_lin.astype(BF16))
    parts.append(drot_ref[0, :, 3 * HD:])
    w = jnp.concatenate([wq_ref[...], wk_ref[...], wv_ref[...]], axis=1)
    acc[...] += dot_nt(jnp.concatenate(parts, axis=1), w)

    @pl.when(g == pl.num_programs(0) - 1)
    def _():
        d_n = acc[...].astype(BF16).astype(F32)
        x = x_ref[0].astype(F32)
        r = lax.rsqrt(jnp.mean(x * x, axis=-1, keepdims=True) + EPSILON)
        dng_ref[...] = jnp.sum(d_n * (x * r), axis=0, keepdims=True)
        scaled = d_n * ng_ref[...]
        dot_mean = jnp.mean(scaled * x, axis=-1, keepdims=True)
        gx_ref[0] = (gy_ref[0].astype(F32) + r * scaled - x * (r * r * r * dot_mean)).astype(BF16)


def grad_tokens(drot, lin, seq, w_query, w_key, w_value, cos, sin, qg, kg, x, gy, ng, so_far):
    groups, toks, _ = drot.shape
    dim = x.shape[2]
    own = pl.BlockSpec((1, toks, dim), lambda g: (seq, 0, 0))
    extra = () if so_far is None else (so_far,)
    full = lambda g: (0, 0)
    col = lambda g: (0, g)
    return pl.pallas_call(
        gradx_kernel,
        grid=(groups,),
        in_specs=[pl.BlockSpec((1, toks, 4 * HD), lambda g: (g, 0, 0)), pl.BlockSpec((1, toks, 3 * HD), lambda g: (g, seq, 0)),
                  pl.BlockSpec((dim, 2 * HD), col), pl.BlockSpec((dim, HD), col), pl.BlockSpec((dim, HD), col),
                  pl.BlockSpec((toks, HD), full), pl.BlockSpec((toks, HD), full), pl.BlockSpec((1, HD), full),
                  pl.BlockSpec((1, HD), full), own, own,
                  pl.BlockSpec((1, dim), full)] + [pl.BlockSpec(memory_space=pl.ANY)] * len(extra),
        out_specs=[own, pl.BlockSpec((1, dim), full)],
        out_shape=[jax.ShapeDtypeStruct(x.shape, BF16), jax.ShapeDtypeStruct((1, dim), F32)],
        input_output_aliases={12: 0} if extra else {},
        scratch_shapes=[pltpu.VMEM((toks, dim), F32)],
        compiler_params=pltpu.CompilerParams(vmem_limit_bytes=VMEM_LIMIT),
        cost_estimate=pl.CostEstimate(flops=2 * toks * dim * 4 * HD * groups, bytes_accessed=40_000_000, transcendentals=0),
        name='grad_tokens',
    )(drot, lin, w_query, w_key, w_value, cos, sin, qg, kg, x, gy, ng, *extra)


def alloc(shape, dtype):
    return pl.pallas_call(lambda out_ref: None, out_specs=pl.BlockSpec(memory_space=pl.ANY),
                          out_shape=jax.ShapeDtypeStruct(shape, dtype), name='alloc')()


def rope_tables(positions):
    half_dim = HD // 2
    inv_freq = ROPE_THETA ** (-jnp.arange(half_dim, dtype=F32) / half_dim)
    angles = positions.astype(F32)[..., None] * inv_freq
    cos, sin = jnp.cos(angles), jnp.sin(angles)
    return jnp.concatenate([cos, cos], axis=-1), jnp.concatenate([-sin, sin], axis=-1)


def solution(mesh):
    n_dev = mesh.shape[SEQ_AXIS]
    tok_spec = P(None, SEQ_AXIS, None)
    pos_spec = P(None, SEQ_AXIS)

    def swap(x, dist):
        return lax.ppermute(x, SEQ_AXIS, [(d, d ^ dist) for d in range(n_dev)])

    def device_fn(x_in, grad_y, positions, norm_gain, w_query, w_key, w_value, w_out, q_gain, k_gain):
        n_batch, seq_dev, dim = x_in.shape
        me = lax.axis_index(SEQ_AXIS)
        seq_len = seq_dev * n_dev
        ng = norm_gain.astype(F32)[None]
        qg = q_gain.astype(F32)[None]
        kg = k_gain.astype(F32)[None]

        x32 = x_in.astype(F32)
        normed = (x32 * lax.rsqrt(jnp.mean(x32 * x32, axis=-1, keepdims=True) + EPSILON) * ng).astype(BF16)

        def after(values, *waits):
            return lax.optimization_barrier((values, waits))[0]

        pos_all = alloc((n_batch, seq_len), jnp.int32)
        for dist in range(n_dev):
            pos_all = lax.dynamic_update_slice(pos_all, swap(positions, dist) if dist else positions, (0, (me ^ dist) * seq_dev))
        normed = after(normed, pos_all)
        n_all = [lax.all_gather(normed[b], SEQ_AXIS, axis=0, tiled=True) for b in range(n_batch)]
        cos_all, sin_all = rope_tables(pos_all)
        cos_own, sin_own = rope_tables(positions)
        own_cols = lambda w, width: lax.dynamic_slice_in_dim(w, me * width, width, axis=1)
        w_own = jnp.concatenate([own_cols(w_query, 2 * HD), own_cols(w_key, HD), own_cols(w_value, HD)], axis=1)

        def col_block(a, dev):
            return lax.dynamic_slice_in_dim(a, dev * 2 * HD, 2 * HD, axis=1)

        def row_block(a, dev):
            return lax.dynamic_slice_in_dim(a, dev * seq_dev, seq_dev, axis=0)

        def exchange(src, cut, put, got, window):
            here, src = lax.optimization_barrier((me, src))
            blocks = [cut(src, here ^ dist) for dist in range(1, n_dev)]
            came = [swap(blk, dist) for dist, blk in enumerate(blocks, 1)]
            came = after([cut(src, here)] + came, window)
            for dist in range(n_dev):
                got = put(got, came[dist], me ^ dist)
            return got

        gy_cat = grad_y.reshape(n_batch * seq_dev, dim)
        d_attn = dot_nt(gy_cat, w_out).astype(BF16)
        n_first, cos_all, sin_all, _ = lax.optimization_barrier((n_all[0], cos_all, sin_all, d_attn))
        n_in = [n_first, n_all[1], n_all[2]]
        saved, outs = [], []
        for b in range(n_batch):
            q, qt, k, kt, v, vt, lin = project(n_in[b], w_own, cos_all[b], sin_all[b], qg, kg)
            o, ot, lse = attend(qt, k, vt)
            saved.append((ot, lse, q, qt, k, kt, v, lin))
            outs.append(o)
            if b == 0:
                lin_own = own_lin(after(normed, lse).reshape(n_batch * seq_dev, dim), w_query, w_key)
                n_in[1] = after(n_in[1], lin_own)

        put_do = lambda got, blk, dev: lax.dynamic_update_slice(got, blk.reshape(n_batch, seq_dev, 2 * HD), (0, dev * seq_dev, 0))
        do_src = after(d_attn, saved[1][1])
        do_all = exchange(do_src, col_block, put_do, alloc((n_batch, seq_len, 2 * HD), BF16), saved[2][1])

        def take_o(b, o_cat, window):
            put = lambda got, blk, dev: lax.dynamic_update_slice(got, blk, (b * seq_dev, dev * 2 * HD))
            return exchange(outs[b], row_block, put, o_cat, window)

        def take_drot(drot, window):
            put = lambda got, blk, dev: lax.dynamic_update_slice(got, blk[None], (dev, 0, 0))
            return exchange(drot, row_block, put, alloc((n_dev, seq_dev, 4 * HD), BF16), window)

        def back(b, waits):
            ot, lse, q, qt, k, kt, v, lin = saved[b]
            q = after(q, waits)
            drot, dlin, dqg, dkg = attend_back(q, qt, do_all, b, ot, lse, k, kt, v, lin, cos_all[b], sin_all[b], qg, kg)
            dw = lax.dot_general(n_all[b], dlin, (((0,), (0,)), ((), ())), preferred_element_type=F32)
            return drot, dqg, dkg, dw

        def to_tokens(b, got, so_far):
            return grad_tokens(got, lin_own, b, w_query, w_key, w_value, cos_own[b], sin_own[b], qg, kg,
                               x_in, grad_y, ng, so_far)

        o_cat = alloc((n_batch * seq_dev, n_dev * 2 * HD), BF16)
        o_cat = take_o(0, o_cat, saved[2][1])
        o_cat = take_o(1, o_cat, saved[2][1])
        o_cat = take_o(2, o_cat, ())
        part = lax.dot_general(o_cat, gy_cat, (((0,), (0,)), ((), ())), preferred_element_type=F32)
        grad_w_out = lax.psum_scatter(part, SEQ_AXIS, scatter_dimension=0, tiled=True)
        drot0, dqg0, dkg0, dw0 = back(0, part)
        drot1, dqg1, dkg1, dw1 = back(1, dw0)
        dw01 = dw0 + dw1
        y_out = (x32.reshape(n_batch * seq_dev, dim) + dot_nn(after(o_cat, dw01), w_out)).astype(BF16).reshape(x_in.shape)
        grad_w_out = lax.all_gather(after(grad_w_out, (y_out, dw01)), SEQ_AXIS, axis=0, tiled=True)
        got0 = take_drot(drot0, drot1)
        drot2, dqg2, dkg2, dw2 = back(2, (dw01, y_out))
        dw_sum, grad_w_out = lax.optimization_barrier((dw01 + dw2, grad_w_out))
        dw_q, dw_kv = dw_sum[:, :2 * HD], dw_sum[:, 2 * HD:]
        got1 = take_drot(drot1, drot2)
        grad_x, dng0 = to_tokens(0, after(got0, (dw_q, dw_kv)), None)
        grad_x, dng1 = to_tokens(1, got1, grad_x)
        grad_x, dng2 = to_tokens(2, take_drot(drot2, grad_x), grad_x)
        dng_sum, dqg_sum, dkg_sum = dng0 + dng1 + dng2, dqg0 + dqg1 + dqg2, dkg0 + dkg1 + dkg2

        def gather_cols(own):
            return jnp.moveaxis(lax.all_gather(own, SEQ_AXIS, axis=0), 0, 1).reshape(dim, -1)

        grad_w_query = gather_cols(dw_q)
        dw_kv = lax.all_gather(after(dw_kv, dng1), SEQ_AXIS, axis=0)
        grad_w_key = jnp.moveaxis(dw_kv[:, :, :HD], 0, 1).reshape(dim, -1)
        grad_w_value = jnp.moveaxis(dw_kv[:, :, HD:], 0, 1).reshape(dim, -1)

        small = jnp.concatenate([dng_sum, dqg_sum, dkg_sum], axis=1)
        for dist in (1, 2, 4):
            small = small + swap(small, dist)
        small = small[0]
        return (y_out, grad_x, small[:dim], grad_w_query, grad_w_key, grad_w_value, grad_w_out,
                small[dim:dim + HD], small[dim + HD:])

    in_specs = (tok_spec, tok_spec, pos_spec, P(), P(), P(), P(), P(), P(), P())
    out_specs = (tok_spec, tok_spec, P(), P(), P(), P(), P(), P(), P())
    return jax.shard_map(device_fn, mesh=mesh, in_specs=in_specs, out_specs=out_specs, check_vma=False)
```
